32 devices in a mesh: tok: 16 (over z, y, x), col: 2 (over core).
Axes of the slice: x: 2, y: 2, z: 4, core: 2. Of those that a mesh axis runs over, the one named last changes fastest.
Arguments:
- first_acts: bfloat16 [24576, 4096], P('tok', 'col'), as said below
- second_acts: bfloat16 [24576, 4096], P('tok', 'col'), as said below
- window_counts: int32 [64], P('tok'), may hold values from 96 to 384, as said below
Outputs:
- whitened: float32 [4096, 4096], P('tok', 'col')
- means: float32 [2, 4096], P(None, 'col')
The draws below stay inside these ranges and needn't reach their ends.
Inputs may be any that keep to these rules, and one draw needn't show every extreme that they name: `window_counts`: the live tokens of a window are its first ones; on every index of tok one of its 4 windows is full with 384 live tokens. `first_acts`: real values of order one to some tens; slots that are not live hold values too. `second_acts`: real values of order one to some tens; slots that are not live hold values too.
All inputs are finite; a program needn't handle non-finite values.
Results may differ from the reference program's by a relative error of at most 0.0003.
Values may be sent and summed in bfloat16 or wider, within the bound.
A program may use at most 192 MiB of HBM per device.

```python
import math
import jax
import jax.numpy as jnp
from jax import lax

D = 4096
WINDOWS = 4
SLOTS = 384
TOK_DEV = 1536
TOKENS = 24576
BLOCKS = 64
N_TOK = 16


def paired_draw(key):
    key = jax.random.fold_in(key, 11)
    streams = jax.random.split(key, 8)
    feature_block = D // N_TOK
    base_field = jax.random.normal(streams[0], (TOKENS, D), jnp.float32)
    noise_field = jax.random.normal(streams[1], (TOKENS, D), jnp.float32)
    offset_scale = 1.0
    common_shift = 0.0
    row_scale = jnp.ones((TOKENS,), jnp.float32)
    channel_scale = jnp.exp(jax.random.uniform(streams[2], (D,), jnp.float32, math.log(0.5), math.log(2.0)))
    block_shift = offset_scale * jax.random.normal(streams[3], (BLOCKS, D), jnp.float32) + common_shift
    second_shift = offset_scale * jax.random.normal(streams[6], (BLOCKS, D), jnp.float32)
    pairing = jax.random.permutation(streams[4], N_TOK)
    row_device = jnp.arange(TOKENS, dtype=jnp.int32) // TOK_DEV
    feature_owner = jnp.arange(D, dtype=jnp.int32) // feature_block
    spike_scale = jnp.where(pairing[row_device][:, None] == feature_owner[None, :], 5.0, 1.0)
    first_field = (base_field * channel_scale[None, :] * row_scale[:, None] + jnp.repeat(block_shift, SLOTS, axis=0)) * spike_scale
    second_field = 0.5 * first_field + 0.4 * jnp.roll(first_field, 1, axis=1) + 0.6 * noise_field * channel_scale[None, :] + jnp.repeat(second_shift, SLOTS, axis=0)
    return (first_field, second_field)


def draw_first_acts(key, part):
    return paired_draw(key)[0].astype(jnp.bfloat16)


def draw_second_acts(key, part):
    return paired_draw(key)[1].astype(jnp.bfloat16)


def draw_window_counts(key, part):
    key_counts, key_full = jax.random.split(jax.random.fold_in(key, 29))
    drawn = jax.random.randint(key_counts, (BLOCKS,), SLOTS // 4, SLOTS + 1, jnp.int32)
    chosen = jax.random.randint(key_full, (N_TOK,), 0, WINDOWS, jnp.int32)
    filled = (lax_iota_windows()[None, :] == chosen[:, None]).reshape(BLOCKS)
    return jnp.where(filled, SLOTS, drawn).astype(jnp.int32)


def lax_iota_windows():
    return jnp.arange(WINDOWS, dtype=jnp.int32)


def setup_inputs(seed: int = 0) -> dict:
    key_of = jax.random.split(jax.random.key(seed), 4)
    first_acts = draw_first_acts(jax.random.fold_in(key_of[3], 71), 0)
    second_acts = draw_second_acts(jax.random.fold_in(key_of[3], 71), 0)
    window_counts = draw_window_counts(jax.random.fold_in(key_of[3], 71), 0)
    return {"first_acts": first_acts, "second_acts": second_acts, "window_counts": window_counts}


def reference(first_acts, second_acts, window_counts):
    blocks = window_counts.shape[0]
    first_win = first_acts.reshape(blocks, SLOTS, D)
    second_win = second_acts.reshape(blocks, SLOTS, D)
    live_mask = lax.broadcasted_iota(jnp.int32, (blocks, SLOTS), 1) < window_counts[:, None]
    count_float = window_counts.astype(jnp.float32)
    mean_first = lax.optimization_barrier(jnp.sum(jnp.where(live_mask[:, :, None], first_win.astype(jnp.float32), 0.0), axis=1)) / count_float[:, None]
    mean_second = lax.optimization_barrier(jnp.sum(jnp.where(live_mask[:, :, None], second_win.astype(jnp.float32), 0.0), axis=1)) / count_float[:, None]
    grand_count = jnp.sum(count_float)
    grand_first = lax.optimization_barrier(jnp.sum(count_float[:, None] * mean_first, axis=0)) / grand_count
    grand_second = lax.optimization_barrier(jnp.sum(count_float[:, None] * mean_second, axis=0)) / grand_count

    def accumulate(carry, inputs):
        cross, square_first, square_second = carry
        rows_first, rows_second, live_rows, win_first, win_second = inputs
        centered_first = jnp.where(live_rows[:, None], rows_first - win_first[None, :], 0.0).astype(jnp.bfloat16)
        centered_second = jnp.where(live_rows[:, None], rows_second - win_second[None, :], 0.0).astype(jnp.bfloat16)
        cross = cross + jnp.dot(centered_first.T, centered_second, preferred_element_type=jnp.float32)
        square_first = square_first + lax.optimization_barrier(jnp.sum(jnp.square(centered_first.astype(jnp.float32)), axis=0))
        square_second = square_second + lax.optimization_barrier(jnp.sum(jnp.square(centered_second.astype(jnp.float32)), axis=0))
        return ((cross, square_first, square_second), None)
    start_state = (jnp.zeros((D, D), jnp.float32), jnp.zeros((D,), jnp.float32), jnp.zeros((D,), jnp.float32))
    (cross, square_first, square_second), _ = lax.scan(accumulate, start_state, (first_win, second_win, live_mask, mean_first, mean_second))
    shift_first = mean_first - grand_first[None, :]
    shift_second = mean_second - grand_second[None, :]
    cross = cross + jnp.dot((count_float[:, None] * shift_first).T, shift_second, preferred_element_type=jnp.float32, precision=lax.Precision.HIGHEST)
    var_first = (square_first + lax.optimization_barrier(jnp.sum(count_float[:, None] * jnp.square(shift_first), axis=0))) / grand_count
    var_second = (square_second + lax.optimization_barrier(jnp.sum(count_float[:, None] * jnp.square(shift_second), axis=0))) / grand_count
    whitened = cross / grand_count / jnp.sqrt((var_first[:, None] + 0.1) * (var_second[None, :] + 0.1))
    means = jnp.stack([grand_first, grand_second])
    return (whitened, means)
```

```python
import jax
import jax.numpy as jnp
from jax import lax
from jax.sharding import PartitionSpec as P

contract_rows = (((0,), (0,)), ((), ()))
COLUMN_CHUNKS = 4


def window_stats(acts, live_mask, count_float):
    windows, slot_count = live_mask.shape
    width = acts.shape[1]
    win = acts.reshape(windows, slot_count, width)
    mean = (
        jnp.einsum(
            "ws,wsd->wd", live_mask.astype(jnp.bfloat16), win, preferred_element_type=jnp.float32
        )
        / count_float[:, None]
    )
    centered = jnp.where(live_mask[:, :, None], win - mean[:, None, :], 0.0).astype(jnp.bfloat16)
    centered = centered.reshape(windows * slot_count, width)
    square = jnp.sum(jnp.square(centered.astype(jnp.float32)), axis=0)
    return mean, centered, square


def local(first_acts, second_acts, window_counts):
    windows = window_counts.shape[0]
    tokens, width = first_acts.shape
    slot_count = tokens // windows
    n = lax.axis_size("tok")
    bits = n.bit_length() - 1
    tok = lax.axis_index("tok")
    col = lax.axis_index("col")
    row_width = 2 * width // n
    unscale = float(1 << max((tokens * n - 1).bit_length() - 2, 0))
    scale = 1.0 / unscale

    peer_acts = lax.ppermute(first_acts, "col", [(0, 1), (1, 0)])
    count_float = window_counts.astype(jnp.float32)
    live_mask = lax.broadcasted_iota(jnp.int32, (windows, slot_count), 1) < window_counts[:, None]
    mean_second, centered_second, square_second = window_stats(second_acts, live_mask, count_float)
    mean_own, centered_own, square_own = window_stats(first_acts, live_mask, count_float)
    mean_peer, centered_peer, square_peer = window_stats(peer_acts, live_mask, count_float)

    def exchange(keep, send, bit):
        coded = (send * scale).astype(jnp.float16)
        got = lax.ppermute(coded, "tok", [(i, i ^ (1 << bit)) for i in range(n)])
        return keep + got.astype(jnp.float32) * unscale

    plain = list(range(bits - 1))
    early = plain[:]
    if len(early) >= 3:
        early[1], early[2] = early[2], early[1]
    swap = {0: 1, 1: 0} if len(early) >= 2 else {0: 0}
    other = [swap.get(b, b) for b in early]
    chunk = width // COLUMN_CHUNKS

    def reduce_half(centered, c):
        order = early if c % 2 == 0 else other
        part = lax.dot_general(
            centered,
            lax.slice_in_dim(centered_second, c * chunk, (c + 1) * chunk, axis=1),
            contract_rows,
            preferred_element_type=jnp.float32,
        )
        part = part.reshape((2,) * (bits - 1) + (row_width, chunk))
        left = plain[::-1]
        for bit in order:
            axis = left.index(bit)
            mine = (tok >> bit) & 1
            keep = lax.dynamic_index_in_dim(part, mine, axis, keepdims=False)
            send = lax.dynamic_index_in_dim(part, 1 - mine, axis, keepdims=False)
            part = exchange(keep, send, bit)
            left.remove(bit)
        return part

    top = tok >> (bits - 1)
    owns = top == col
    owned = [reduce_half(centered_own, c) for c in range(COLUMN_CHUNKS)]
    peered = [reduce_half(centered_peer, c) for c in range(COLUMN_CHUNKS)]
    within = jnp.concatenate(
        [
            exchange(jnp.where(owns, a, b), jnp.where(owns, b, a), bits - 1)
            for a, b in zip(owned, peered)
        ],
        axis=1,
    )

    count_row = jnp.pad(count_float, (0, width - windows))
    packed = jnp.concatenate(
        [
            mean_own,
            mean_peer,
            mean_second,
            square_own[None],
            square_peer[None],
            square_second[None],
            count_row[None],
        ],
        axis=0,
    )
    every = lax.all_gather(packed, "tok", axis=0, tiled=False)
    counts = every[:, 3 * windows + 3, :windows].reshape(n * windows)
    grand_count = jnp.sum(counts)

    def merged(means, squares):
        means = means.reshape(n * windows, means.shape[-1])
        grand = jnp.sum(counts[:, None] * means, axis=0) / grand_count
        shift = means - grand[None, :]
        spread = jnp.sum(squares, axis=0) + jnp.sum(counts[:, None] * jnp.square(shift), axis=0)
        return grand, shift, spread / grand_count

    offset = (tok & (n // 2 - 1)) * row_width
    squares_at = 3 * windows
    rows_means = lax.dynamic_slice_in_dim(
        jnp.where(owns, every[:, :windows], every[:, windows : 2 * windows]), offset, row_width, 2
    )
    rows_squares = lax.dynamic_slice_in_dim(
        jnp.where(owns, every[:, squares_at], every[:, squares_at + 1]), offset, row_width, 1
    )
    _, shift_rows, var_rows = merged(rows_means, rows_squares)
    grand_second, shift_second, var_second = merged(
        every[:, 2 * windows : 3 * windows], every[:, squares_at + 2]
    )
    own_means = every[:, :windows].reshape(n * windows, width)
    grand_first = jnp.sum(counts[:, None] * own_means, axis=0) / grand_count
    between = lax.dot_general(
        counts[:, None] * shift_rows,
        shift_second,
        contract_rows,
        precision=lax.Precision.HIGHEST,
        preferred_element_type=jnp.float32,
    )
    whitened = (
        (within + between)
        / grand_count
        / jnp.sqrt((var_rows[:, None] + 0.1) * (var_second[None, :] + 0.1))
    )
    return (whitened, jnp.stack([grand_first, grand_second]))


def solution(mesh):
    placed = (P("tok", "col"), P("tok", "col"), P("tok"))
    return jax.shard_map(
        local,
        mesh=mesh,
        in_specs=placed,
        out_specs=(P("tok", "col"), P(None, "col")),
        check_vma=False,
    )
```
